32 devices in a mesh: lat: 8 (over y, x, core), lon: 4 (over z).
Axes of the slice: x: 2, y: 2, z: 4, core: 2. Of those that a mesh axis runs over, the one named last changes fastest.
Arguments:
- loadings: float32 [176, 720, 200], P('lat', 'lon'), may hold values from -60 to 60, as said below
Outputs:
- rotated: float32 [176, 720, 200], P('lat', 'lon')
- rotation: float32 [200, 200], replicated
The draws below stay inside these ranges and needn't reach their ends.
Inputs may be any that keep to these rules, and one draw needn't show every extreme that they name: Every grid point's loadings are not all zero.
All inputs are finite; a program needn't handle non-finite values.
Results may differ from the reference program's by a relative error of at most 0.00011.
Values sent between devices are 32-bit elements; how exact they have to be, the bound alone decides.
No kernel may reach another device: no remote copies, remote signals or barrier semaphores. Data moves between devices by JAX's collectives and lax.ppermute only.
A program may use at most 64 MiB of HBM per device.

```python
import math
import jax
import jax.numpy as jnp
from jax import lax

K = 200
LAT_DEV = 22
SWEEPS = 2
NS_STEPS = 20
NLAT = 176
NLON = 720
N_LAT = 8


def draw_loadings(key, part):
    base_key = jax.random.fold_in(key, 17)
    keys = jax.random.split(base_key, 8)
    rows = jnp.arange(NLAT).astype(jnp.int32)[:, None]
    cols = jnp.arange(NLON).astype(jnp.int32)[None, :]
    region = rows * 10 // NLAT * 20 + cols * 20 // NLON
    order = jax.random.permutation(keys[0], K).astype(jnp.int32)
    primary = order[region % K]
    secondary = order[(region + 20 + rows % 3) % K]
    flips = jax.random.randint(keys[1], (NLAT, NLON, 1), 0, 2).astype(jnp.float32) * 2.0 - 1.0
    modes = jnp.arange(K).astype(jnp.int32)[None, None, :]
    noise = 0.25 * jnp.clip(jax.random.normal(keys[2], (NLAT, NLON, K), jnp.float32), -3.0, 3.0)
    strength = 2.0 + jnp.abs(jnp.clip(jax.random.normal(keys[3], (NLAT, NLON, 1), jnp.float32), -3.0, 3.0))
    row_scale = jnp.exp(jax.random.uniform(keys[5], (NLAT, NLON, 1), jnp.float32) * math.log(10.0))
    side = 0.5 * strength * jax.random.uniform(keys[4], (NLAT, NLON, 1), jnp.float32, -1.0, 1.0)
    structure = noise + jnp.where(modes == primary[:, :, None], flips * strength, 0.0)
    structure = structure + jnp.where(modes == secondary[:, :, None], side, 0.0)
    col_scale = jnp.exp(jax.random.uniform(keys[6], (1, 1, K), jnp.float32, -1.0, 0.0) * math.log(3.0))
    structure = structure * row_scale * col_scale
    gauss = jax.random.normal(keys[7], (K, K), jnp.float32)
    ortho, upper = jnp.linalg.qr(gauss)
    ortho = ortho * jnp.where(jnp.diagonal(upper) >= 0.0, 1.0, -1.0)[None, :]
    mixed = jnp.dot(structure.reshape(NLAT * NLON, K), ortho, precision=lax.Precision.HIGHEST)
    return jnp.clip(mixed.reshape(NLAT, NLON, K), -60.0, 60.0)


def setup_inputs(seed: int = 0) -> dict:
    key_list = jax.random.split(jax.random.key(seed), 2)
    loadings = draw_loadings(jax.random.fold_in(key_list[1], 71), 0)
    return dict(loadings=loadings)


def grid_weights():
    rows = jnp.arange(NLAT).astype(jnp.float32)
    degrees = -90.0 + (rows + 0.5) * (180.0 / NLAT)
    return jnp.cos(degrees * (math.pi / 180.0))

def matmul(left, right):
    return jnp.dot(left, right, precision=lax.Precision.HIGHEST)

def polar_factor(gradient):
    iterate = gradient / jnp.sqrt(jnp.sum(gradient * gradient))
    for count in range(NS_STEPS):
        iterate = 1.5 * iterate - 0.5 * matmul(iterate, matmul(iterate.T, iterate))
    return iterate

def reference(loadings):
    row_norm = jnp.sqrt(lax.optimization_barrier(jnp.sum(loadings * loadings, axis=-1, keepdims=True)) + 1e-06)
    normed = loadings / row_norm
    weights = grid_weights()
    total = jnp.sum(weights) * NLON
    bands = normed.reshape(N_LAT, LAT_DEV * NLON, K)
    band_weights = jnp.repeat(weights.reshape(N_LAT, LAT_DEV), NLON, axis=1).reshape(N_LAT, LAT_DEV * NLON, 1)
    rotation = jnp.eye(K, dtype=jnp.float32)
    for sweep_index in range(SWEEPS):

        def colsq_band(carry, pair):
            block, block_weights = pair
            spun = matmul(block, rotation)
            return (carry + lax.optimization_barrier(jnp.sum(block_weights * spun * spun, axis=0)), None)
        colsq, unused = lax.scan(colsq_band, jnp.zeros((K,), jnp.float32), (bands, band_weights))

        def gradient_band(carry, pair):
            block, block_weights = pair
            spun = matmul(block, rotation)
            term = block_weights * (spun * spun * spun - spun * (colsq / total)[None, :])
            return (carry + matmul(block.T, term), None)
        gradient, unused = lax.scan(gradient_band, jnp.zeros((K, K), jnp.float32), (bands, band_weights))
        rotation = polar_factor(gradient)
    flat = normed.reshape(NLAT * NLON, K)
    rotated = matmul(flat, rotation).reshape(NLAT, NLON, K) * row_norm
    return (rotated, rotation)
```

```python
import functools
import math

import jax
import jax.numpy as jnp
from jax import lax
from jax.experimental import pallas as pl
from jax.experimental.pallas import tpu as pltpu
from jax.sharding import PartitionSpec as P

SWEEPS = 2
NS_STEPS = 20
AXES = ("lat", "lon")
F32 = jnp.float32
BF16 = jnp.bfloat16


def latitude_weight(rows, lat_total):
    degrees = -90.0 + (rows.astype(jnp.float32) + 0.5) * (180.0 / lat_total)
    return jnp.cos(degrees * (math.pi / 180.0))


def halves(value):
    high = value.astype(BF16)
    return high, (value - high.astype(F32)).astype(BF16)


def dot_nn(left, right):
    return lax.dot_general(left, right, (((1,), (0,)), ((), ())), preferred_element_type=F32)


def dot_nt(left, right):
    return lax.dot_general(left, right, (((1,), (1,)), ((), ())), preferred_element_type=F32)


def triple(dot, left, right):
    return dot(left[0], right[0]) + (dot(left[0], right[1]) + dot(left[1], right[0]))


def polar_transposed(gradient):
    iterate = gradient / jnp.sqrt(jnp.sum(gradient * gradient))

    def step(_, current):
        parts = halves(current)
        inner = triple(dot_nt, parts, parts)
        return 1.5 * current - 0.5 * triple(dot_nn, halves(inner), parts)

    return lax.fori_loop(0, NS_STEPS, step, iterate)


def group_of(lat_rows):
    return max(d for d in range(1, min(lat_rows, 11) + 1) if lat_rows % d == 0)


def normalize_rows(x_ref, first, count, stage):
    cols = x_ref.shape[1]
    pad = stage.shape[0] // count
    for r in range(count):
        x = x_ref[first + r]
        norm = jnp.sqrt(jnp.sum(x * x, axis=-1, keepdims=True) + 1e-06)
        stage[r * pad:r * pad + cols, :] = x * (1.0 / norm)


def products(left, parts):
    return triple(dot_nn, halves(left), parts)


def first_kernel(x_ref, w_ref, out_ref, stage, *, count):
    step = pl.program_id(0)

    @pl.when(step == 0)
    def _():
        stage[...] = jnp.zeros_like(stage)
        out_ref[...] = jnp.zeros_like(out_ref)

    normalize_rows(x_ref, 0, count, stage)
    normed = stage[...]
    parts = halves(normed)
    flipped = normed.T
    weighted = flipped * w_ref[0]
    modes = normed.shape[1]
    out_ref[0, 0:modes, :] += products(weighted, parts)
    out_ref[1, 0:modes, :] += products(weighted * flipped * flipped, parts)


def diagonal(square):
    rows = lax.broadcasted_iota(jnp.int32, square.shape, 0)
    cols = lax.broadcasted_iota(jnp.int32, square.shape, 1)
    return jnp.sum(jnp.where(rows == cols, square, 0.0), axis=1, keepdims=True)


def middle_kernel(total_ref, sums_ref, w_ref, x_hbm, out_ref, rot_ref, x_ref, stage, sem, *, count):
    copy = pltpu.make_async_copy(x_hbm, x_ref, sem)
    copy.start()
    modes = x_ref.shape[2]
    gram = sums_ref[0, 0:modes, :]
    cubic = sums_ref[1, 0:modes, :]
    rotation = polar_transposed(cubic - gram * (diagonal(gram) / total_ref[0]))
    rot_ref[...] = rotation
    stage[...] = jnp.zeros_like(stage)
    out_ref[...] = jnp.zeros_like(out_ref)
    copy.wait()
    rot_parts = halves(rotation)

    def body(step, _):
        normalize_rows(x_ref, step * count, count, stage)
        parts = halves(stage[...])
        spun = triple(dot_nt, rot_parts, parts)
        cubed = spun * spun * spun * w_ref[step]
        out_ref[0:modes, :] += products(cubed, parts)
        return 0

    lax.fori_loop(0, x_ref.shape[0] // count, body, 0)


def last_kernel(total_ref, gram_ref, old_ref, cubic_ref, x_hbm, out_hbm, rot_ref, x_ref, out_ref, sem, sems):
    copy = pltpu.make_async_copy(x_hbm, x_ref, sem)
    copy.start()
    lat_rows, _, modes = x_ref.shape
    old = old_ref[...]
    turned = triple(dot_nn, halves(old), halves(gram_ref[0, 0:modes, :]))
    colsq = jnp.sum(turned * old, axis=1, keepdims=True)
    rotation = polar_transposed(cubic_ref[0:modes, :] - turned * (colsq / total_ref[0]))
    rot_ref[...] = rotation.T
    parts = halves(rotation)
    copy.wait()
    writes = []
    for r in range(lat_rows):
        out_ref[r] = triple(dot_nt, halves(x_ref[r]), parts)
        write = pltpu.make_async_copy(out_ref.at[r], out_hbm.at[r], sems.at[r])
        write.start()
        writes.append(write)
    for write in writes:
        write.wait()


def exchange_sum(value):
    lon = lax.axis_size("lon")
    lat = lax.axis_size("lat")
    devices = lat * lon

    def send(data, lat_mask, lon_mask):
        pairs = [(i, ((i // lon) ^ lat_mask) * lon + ((i % lon) ^ lon_mask)) for i in range(devices)]
        return lax.ppermute(data, AXES, pairs)

    dim = value.ndim - 2
    half = value.shape[dim] // 2
    core = lax.axis_index("lat") % 2
    kept = lax.dynamic_slice_in_dim(value, core * half, half, dim)
    sent = lax.dynamic_slice_in_dim(value, (1 - core) * half, half, dim)
    part = kept + send(sent, 1, 0)
    for bit in range(1, lat.bit_length() - 1):
        part = part + send(part, 1 << bit, 0)
    for bit in range(lon.bit_length() - 1):
        part = part + send(part, 0, (1 << (bit + 1)) - 1)
    other = send(part, 1, 0)
    low = jnp.where(core == 0, part, other)
    high = jnp.where(core == 0, other, part)
    return jnp.concatenate([low, high], axis=dim)


def shards(loadings):
    lat_rows, lon_cols, modes = loadings.shape
    lat_total = lat_rows * lax.axis_size("lat")
    lon_total = lon_cols * lax.axis_size("lon")
    count = group_of(lat_rows)
    steps = lat_rows // count
    pad = -(-lon_cols // 8) * 8
    tall = -(-modes // 16) * 16
    own_rows = lax.axis_index("lat") * lat_rows + jnp.arange(lat_rows)
    weights = latitude_weight(own_rows, lat_total)
    weight_lanes = jnp.repeat(weights, pad).reshape(steps, 1, count * pad)
    total = (jnp.sum(latitude_weight(jnp.arange(lat_total), lat_total)) * lon_total).reshape(1)
    stage = pltpu.VMEM((count * pad, modes), F32)
    vmem = pl.BlockSpec(memory_space=pltpu.VMEM)
    smem = pl.BlockSpec(memory_space=pltpu.SMEM)
    hbm = pl.BlockSpec(memory_space=pl.ANY)
    square = jax.ShapeDtypeStruct((modes, modes), F32)

    sums = pl.pallas_call(
        functools.partial(first_kernel, count=count),
        grid=(steps,),
        in_specs=[
            pl.BlockSpec((count, lon_cols, modes), lambda i: (i, 0, 0)),
            pl.BlockSpec((1, 1, count * pad), lambda i: (i, 0, 0)),
        ],
        out_specs=pl.BlockSpec((2, tall, modes), lambda i: (0, 0, 0)),
        out_shape=jax.ShapeDtypeStruct((2, tall, modes), F32),
        scratch_shapes=[stage],
        name="first_products",
    )(loadings, weight_lanes)
    sums = exchange_sum(sums)

    cubic, rotation = pl.pallas_call(
        functools.partial(middle_kernel, count=count),
        in_specs=[smem, vmem, vmem, hbm],
        out_specs=[vmem, vmem],
        out_shape=[jax.ShapeDtypeStruct((tall, modes), F32), square],
        scratch_shapes=[pltpu.VMEM(loadings.shape, F32), stage, pltpu.SemaphoreType.DMA(())],
        name="polar_and_products",
    )(total, sums, weight_lanes, loadings)
    cubic = exchange_sum(cubic)

    rotated, rotation = pl.pallas_call(
        last_kernel,
        in_specs=[smem, vmem, vmem, vmem, hbm],
        out_specs=[hbm, vmem],
        out_shape=[jax.ShapeDtypeStruct(loadings.shape, F32), square],
        scratch_shapes=[
            pltpu.VMEM(loadings.shape, F32),
            pltpu.VMEM(loadings.shape, F32),
            pltpu.SemaphoreType.DMA(()),
            pltpu.SemaphoreType.DMA((lat_rows,)),
        ],
        name="polar_and_rotate",
    )(total, sums, rotation, cubic, loadings)
    return (rotated, rotation)


def solution(mesh):
    return jax.shard_map(
        shards,
        mesh=mesh,
        in_specs=(P("lat", "lon", None),),
        out_specs=(P("lat", "lon", None), P()),
        check_vma=False,
    )
```

```python
import functools
import math

import jax
import jax.numpy as jnp
import numpy as np
from jax import lax
from jax.experimental import pallas as pl
from jax.experimental.pallas import tpu as pltpu
from jax.sharding import PartitionSpec as P

SWEEPS = 2
NS_STEPS = 20
AXES = ("lat", "lon")
F32 = jnp.float32
BF16 = jnp.bfloat16


def latitude_weight(rows, lat_total):
    degrees = -90.0 + (rows.astype(jnp.float32) + 0.5) * (180.0 / lat_total)
    return jnp.cos(degrees * (math.pi / 180.0))


def halves(value):
    high = value.astype(BF16)
    return high, (value - high.astype(F32)).astype(BF16)


def dot_nn(left, right):
    return lax.dot_general(left, right, (((1,), (0,)), ((), ())), preferred_element_type=F32)


def dot_nt(left, right):
    return lax.dot_general(left, right, (((1,), (1,)), ((), ())), preferred_element_type=F32)


def triple(dot, left, right):
    return dot(left[0], right[0]) + (dot(left[0], right[1]) + dot(left[1], right[0]))


def polar_transposed(gradient):
    iterate = gradient / jnp.sqrt(jnp.sum(gradient * gradient))

    def step(_, current):
        parts = halves(current)
        inner = triple(dot_nt, parts, parts)
        return 1.5 * current - 0.5 * triple(dot_nn, halves(inner), parts)

    return lax.fori_loop(0, NS_STEPS, step, iterate)


def group_of(lat_rows):
    return max(d for d in range(1, min(lat_rows, 11) + 1) if lat_rows % d == 0)


def normalize_rows(x_ref, first, count, stage):
    cols = x_ref.shape[1]
    pad = stage.shape[0] // count
    for r in range(count):
        x = x_ref[first + r]
        norm = jnp.sqrt(jnp.sum(x * x, axis=-1, keepdims=True) + 1e-06)
        stage[r * pad:r * pad + cols, :] = x * (1.0 / norm)


def products(left, parts):
    return triple(dot_nn, halves(left), parts)


def weight_lanes(w_ref, first, count, pad):
    lane = lax.broadcasted_iota(jnp.int32, (1, count * pad), 1)
    lanes = jnp.zeros((1, count * pad), F32)
    for r in range(count):
        lanes = jnp.where(lane >= r * pad, w_ref[first + r], lanes)
    return lanes


def half_of(ref, which):
    rows = ref.shape[0] // 2
    return ref.at[pl.ds(pl.multiple_of(which * rows, 8), rows), :]


def part_out(core_ref, sums_ref, kept_ref, sent_ref):
    kept_ref[...] = half_of(sums_ref, core_ref[0])[...]
    sent_ref[...] = half_of(sums_ref, 1 - core_ref[0])[...]


def put_together(core_ref, own_ref, other_ref, sums_ref):
    half_of(sums_ref, core_ref[0])[...] = own_ref[...]
    half_of(sums_ref, 1 - core_ref[0])[...] = other_ref[...]


def first_kernel(core_ref, w_ref, x_ref, kept_ref, sent_ref, stage, sums, *, count):
    step = pl.program_id(0)

    @pl.when(step == 0)
    def _():
        stage[...] = jnp.zeros_like(stage)
        sums[...] = jnp.zeros_like(sums)

    normalize_rows(x_ref, 0, count, stage)
    normed = stage[...]
    parts = halves(normed)
    flipped = normed.T
    weighted = flipped * weight_lanes(w_ref, step * count, count, stage.shape[0] // count)
    modes = normed.shape[1]
    tall = -(-modes // 8) * 8
    sums[0:modes, :] += products(weighted, parts)
    sums[tall:tall + modes, :] += products(weighted * flipped * flipped, parts)

    @pl.when(step == pl.num_programs(0) - 1)
    def _():
        part_out(core_ref, sums, kept_ref, sent_ref)


def diagonal(square):
    rows = lax.broadcasted_iota(jnp.int32, square.shape, 0)
    cols = lax.broadcasted_iota(jnp.int32, square.shape, 1)
    return jnp.sum(jnp.where(rows == cols, square, 0.0), axis=1, keepdims=True)


def middle_kernel(core_ref, w_ref, own_ref, other_ref, x_hbm, kept_ref, sent_ref, rot_ref, gram_ref,
                  x_ref, stage, sums, cubics, sem, *, count, total):
    copy = pltpu.make_async_copy(x_hbm, x_ref, sem)
    copy.start()
    modes = x_ref.shape[2]
    tall = -(-modes // 8) * 8
    put_together(core_ref, own_ref, other_ref, sums)
    gram = sums[0:modes, :]
    gram_ref[...] = gram
    rotation = polar_transposed(sums[tall:tall + modes, :] - gram * (diagonal(gram) / total))
    rot_ref[...] = rotation
    stage[...] = jnp.zeros_like(stage)
    cubics[...] = jnp.zeros_like(cubics)
    copy.wait()
    rot_parts = halves(rotation)

    def body(step, _):
        normalize_rows(x_ref, step * count, count, stage)
        parts = halves(stage[...])
        spun = triple(dot_nt, rot_parts, parts)
        lanes = weight_lanes(w_ref, step * count, count, stage.shape[0] // count)
        cubics[0:modes, :] += products(spun * spun * spun * lanes, parts)
        return 0

    lax.fori_loop(0, x_ref.shape[0] // count, body, 0)
    part_out(core_ref, cubics, kept_ref, sent_ref)


def last_kernel(core_ref, gram_ref, old_ref, own_ref, other_ref, x_hbm, out_hbm, rot_ref,
                x_ref, out_ref, cubics, sem, sems, *, total):
    copy = pltpu.make_async_copy(x_hbm, x_ref, sem)
    copy.start()
    lat_rows, _, modes = x_ref.shape
    put_together(core_ref, own_ref, other_ref, cubics)
    old = old_ref[...]
    turned = triple(dot_nn, halves(old), halves(gram_ref[...]))
    colsq = jnp.sum(turned * old, axis=1, keepdims=True)
    rotation = polar_transposed(cubics[0:modes, :] - turned * (colsq / total))
    rot_ref[...] = rotation.T
    parts = halves(rotation)
    copy.wait()
    writes = []
    for r in range(lat_rows):
        out_ref[r] = triple(dot_nt, halves(x_ref[r]), parts)
        write = pltpu.make_async_copy(out_ref.at[r], out_hbm.at[r], sems.at[r])
        write.start()
        writes.append(write)
    for write in writes:
        write.wait()


def tree_sum(values):
    while len(values) > 1:
        values = [left + right for left, right in zip(values[::2], values[1::2])]
    return values[0]


def exchange_sum(kept, sent):
    lon = lax.axis_size("lon")
    lat = lax.axis_size("lat")
    devices = lat * lon
    plane = lat // 2
    place = lax.axis_index("lat") // 2
    rows = kept.shape[0] // plane

    def send(data, lat_mask, lon_mask):
        pairs = [(i, ((i // lon) ^ lat_mask) * lon + ((i % lon) ^ lon_mask)) for i in range(devices)]
        return lax.ppermute(data, AXES, pairs)

    part = (kept + send(sent, 1, 0)).reshape(plane, rows, kept.shape[1])

    def chunk(array, mask):
        return lax.dynamic_index_in_dim(array, place ^ mask, 0, keepdims=False)

    own = tree_sum([chunk(part, 0)] + [send(chunk(part, m), 2 * m, 0) for m in range(1, plane)])
    own = tree_sum([own] + [send(own, 0, m) for m in range(1, lon)])
    gathered = jnp.stack([own] + [send(own, 2 * m, 0) for m in range(1, plane)])
    half = jnp.concatenate([chunk(gathered, m) for m in range(plane)])
    return half, send(half, 1, 0)


def shards(loadings):
    lat_rows, lon_cols, modes = loadings.shape
    lat = lax.axis_size("lat")
    lat_total = lat_rows * lat
    lon_total = lon_cols * lax.axis_size("lon")
    count = group_of(lat_rows)
    pad = -(-lon_cols // 8) * 8
    tall = -(-modes // 8) * 8
    own_rows = lax.axis_index("lat") * lat_rows + jnp.arange(lat_rows)
    weights = latitude_weight(own_rows, lat_total)
    degrees = -90.0 + (np.arange(lat_total) + 0.5) * (180.0 / lat_total)
    total = float(np.sum(np.cos(degrees * (math.pi / 180.0)))) * lon_total
    core = (lax.axis_index("lat") % 2).astype(jnp.int32).reshape(1)
    stage = pltpu.VMEM((count * pad, modes), F32)
    whole = pltpu.VMEM(loadings.shape, F32)
    vmem = pl.BlockSpec(memory_space=pltpu.VMEM)
    smem = pl.BlockSpec(memory_space=pltpu.SMEM)
    hbm = pl.BlockSpec(memory_space=pl.ANY)
    square = jax.ShapeDtypeStruct((modes, modes), F32)

    def half_rows(needed):
        return lat // 2 * (-(-needed // (8 * lat)) * 8)

    two, one = half_rows(2 * tall), half_rows(tall)
    half_two = jax.ShapeDtypeStruct((two, modes), F32)
    half_one = jax.ShapeDtypeStruct((one, modes), F32)
    sums = pltpu.VMEM((2 * two, modes), F32)
    cubics = pltpu.VMEM((2 * one, modes), F32)

    kept, sent = pl.pallas_call(
        functools.partial(first_kernel, count=count),
        grid=(lat_rows // count,),
        in_specs=[smem, smem, pl.BlockSpec((count, lon_cols, modes), lambda i: (i, 0, 0))],
        out_specs=[pl.BlockSpec((two, modes), lambda i: (0, 0))] * 2,
        out_shape=[half_two, half_two],
        scratch_shapes=[stage, sums],
        name="first_products",
    )(core, weights, loadings)
    own, other = exchange_sum(kept, sent)

    kept, sent, rotation, gram = pl.pallas_call(
        functools.partial(middle_kernel, count=count, total=total),
        in_specs=[smem, smem, vmem, vmem, hbm],
        out_specs=[vmem] * 4,
        out_shape=[half_one, half_one, square, square],
        scratch_shapes=[whole, stage, sums, cubics, pltpu.SemaphoreType.DMA(())],
        name="polar_and_products",
    )(core, weights, own, other, loadings)
    own, other = exchange_sum(kept, sent)

    rotated, rotation = pl.pallas_call(
        functools.partial(last_kernel, total=total),
        in_specs=[smem, vmem, vmem, vmem, vmem, hbm],
        out_specs=[hbm, vmem],
        out_shape=[jax.ShapeDtypeStruct(loadings.shape, F32), square],
        scratch_shapes=[whole, whole, cubics, pltpu.SemaphoreType.DMA(()), pltpu.SemaphoreType.DMA((lat_rows,))],
        name="polar_and_rotate",
    )(core, gram, rotation, own, other, loadings)
    return (rotated, rotation)


def solution(mesh):
    return jax.shard_map(
        shards,
        mesh=mesh,
        in_specs=(P("lat", "lon", None),),
        out_specs=(P("lat", "lon", None), P()),
        check_vma=False,
    )
```
